32 devices in a mesh: group: 2 (over x), expert: 16 (over z, y, core).
Axes of the slice: x: 2, y: 2, z: 4, core: 2. Of those that a mesh axis runs over, the one named last changes fastest.
Arguments:
- query: bfloat16 [32, 2048], P(('group', 'expert')), parts along dimension 0, may hold values from -600 to 600
- key_new: bfloat16 [32, 2048], P(('group', 'expert')), parts along dimension 0, may hold values from -6 to 6
- value_new: bfloat16 [32, 2048], P(('group', 'expert')), parts along dimension 0, may hold values from -6 to 6
- key_cache: bfloat16 [32, 256, 2048], P(('group', 'expert')), parts along dimension 0, may hold values from -6 to 6
- value_cache: bfloat16 [32, 256, 2048], P(('group', 'expert')), parts along dimension 0, may hold values from -6 to 6
- lengths: int32 [32], P(('group', 'expert')), parts along dimension 0, may hold values from 1 to 256
- hidden: bfloat16 [32, 2048], P(('group', 'expert')), parts along dimension 0, may hold values from -6 to 6
- routes: int32 [32], P('group'), parts along dimension 0, may hold values from 0 to 31, as said below
- w_out: bfloat16 [2048, 2048], P(None, 'expert'), may hold values from -0.125 to 0.125
- ln_gain: bfloat16 [2048], replicated, may hold values from 0.099609375 to 1.8984375
- router: bfloat16 [2048, 32], replicated, may hold values from -0.125 to 0.125
- shared_up: bfloat16 [2048, 8192], P(None, 'expert'), may hold values from -0.125 to 0.125
- shared_down: bfloat16 [8192, 2048], P('expert'), may hold values from -0.0625 to 0.0625
- expert_up: bfloat16 [2048, 131072], P(None, 'expert'), may hold values from -0.125 to 0.125
- expert_down: bfloat16 [131072, 2048], P('expert'), may hold values from -0.09375 to 0.09375
Outputs:
- layer_out: bfloat16 [32, 2048], P(('group', 'expert')), parts along dimension 0
The draws below stay inside these ranges and needn't reach their ends.
There are 2 independent parts, one for each index of `group`. The reference program is written for one: setup_inputs(seed, part) draws one part's arguments, and reference() takes and returns one part's arrays. A program takes and returns all parts, laid end to end along the dimension named above; an argument that names none is the same for every part. Nothing has to cross between parts.
Inputs may be any that keep to these rules, and one draw needn't show every extreme that they name: `routes`: no expert is named by more than 2 tokens of the group, and in every draw some expert is named by exactly 2.
All inputs are finite; a program needn't handle non-finite values.
Results may differ from the reference program's by a relative error of at most 0.0085.
Values may be sent and summed in bfloat16 or wider, within the bound.
A program may use at most 128 MiB of HBM per device.

```python
import math
import jax
import jax.numpy as jnp
from jax import lax

D = 2048
HEADS = 16
HEAD_DIM = 128
FF = 4096
EXPERTS = 32
SHARED_FF = 8192
CACHE = 256
S = 16
CAP = 2


def draw_query(key, part):
    base = jnp.clip(jax.random.normal(key, (S, D), jnp.float32), -6.0, 6.0)
    return base.astype(jnp.bfloat16)


def draw_routes(key, part):
    order_key = jax.random.fold_in(key, 11)
    hot_key = jax.random.fold_in(key, 12)
    second_key = jax.random.fold_in(key, 13)
    count_key = jax.random.fold_in(key, 14)
    shuffle_key = jax.random.fold_in(key, 15)
    offset_key = jax.random.fold_in(key, 16)
    token_order = jax.random.permutation(order_key, S)
    hottest = jax.random.randint(hot_key, (), 0, EXPERTS)
    second = (hottest + 1 + jax.random.randint(second_key, (), 0, EXPERTS - 1)) % EXPERTS
    second_count = jax.random.randint(count_key, (), 1, CAP + 1)
    expert_index = jnp.arange(EXPERTS, dtype=jnp.int32)
    shuffled = jax.random.permutation(shuffle_key, EXPERTS).astype(jnp.int32)
    shuffled = jnp.where(expert_index == hottest, EXPERTS, shuffled)
    shuffled = jnp.where(expert_index == second, EXPERTS + 1, shuffled)
    others = jnp.argsort(shuffled, stable=True).astype(jnp.int32)
    offset = jax.random.randint(offset_key, (), 0, EXPERTS - 2)
    position = jnp.arange(S, dtype=jnp.int32)
    remaining = (position - CAP - second_count + offset) % (EXPERTS - 2)
    chosen = jnp.where(position < CAP, hottest, jnp.where(position < CAP + second_count, second, others[remaining]))
    return jnp.zeros((S,), jnp.int32).at[token_order].set(chosen.astype(jnp.int32))


def place_ends(entries, own_key, smallest, largest):
    shape = entries.shape
    place = [jax.random.randint(jax.random.fold_in(own_key, axis), (), 0, shape[axis]) for axis in range(len(shape))]
    entries = entries.at[tuple(place)].set(smallest)
    longest = shape.index(max(shape))
    place[longest] = (place[longest] + 1) % shape[longest]
    return entries.at[tuple(place)].set(largest)


def block_levels(own_key, shape, pieces, low, top_value):
    loudness = 1.0
    for dim, parts in pieces:
        heights = jax.random.uniform(jax.random.fold_in(jax.random.fold_in(own_key, 6), dim), (parts,), jnp.float32, low / len(pieces), top_value / len(pieces))
        loudness = loudness * jnp.repeat(jnp.exp(heights), shape[dim] // parts).reshape((-1,) + (1,) * (len(shape) - 1 - dim))
    return loudness


def gaussian(stream_key, shape, width, bound, pieces=(), held_as=jnp.bfloat16):
    drawn = jax.random.normal(stream_key, shape, jnp.float32) * width
    if len(pieces) > 0:
        drawn = block_levels(stream_key, shape, pieces, -0.22, 0.18) * drawn
    return jnp.clip(drawn, min=-bound, max=bound).astype(held_as)


def setup_inputs(seed: int = 0, part: int = 0) -> dict:
    keys = jax.random.split(jax.random.key(seed), 16)
    part_splits = jax.random.split(jax.random.fold_in(keys[15], part), 16)
    return {
        "query": draw_query(jax.random.fold_in(jax.random.fold_in(keys[15], part), 71), part),
        "key_new": gaussian(part_splits[1], (S, D), 1.0, 6.0, ((0, 16),)),
        "value_new": gaussian(part_splits[2], (S, D), 1.0, 6.0, ((0, 16),)),
        "key_cache": gaussian(part_splits[3], (S, CACHE, D), 1.0, 6.0, ((0, 16),)),
        "value_cache": gaussian(part_splits[4], (S, CACHE, D), 1.0, 6.0, ((0, 16),)),
        "lengths": place_ends(jax.random.randint(part_splits[5], (S,), 1, CACHE + 1), jax.random.fold_in(part_splits[5], 1), 1, CACHE).astype(jnp.int32),
        "hidden": gaussian(part_splits[6], (S, D), 1.0, 6.0, ((0, 16),)),
        "routes": draw_routes(jax.random.fold_in(jax.random.fold_in(keys[15], part), 71), part),
        "w_out": gaussian(keys[8], (D, D), D ** -0.5, 0.125, ((1, 16),)),
        "ln_gain": jnp.clip(1.0 + 0.18 * jax.random.normal(keys[9], (D,), jnp.float32), 0.099609375, 1.8984375).astype(jnp.bfloat16),
        "router": gaussian(keys[10], (D, EXPERTS), D ** -0.5, 0.125),
        "shared_up": gaussian(keys[11], (D, SHARED_FF), D ** -0.5, 0.125, ((1, 16),)),
        "shared_down": gaussian(keys[12], (SHARED_FF, D), SHARED_FF ** -0.5, 0.0625, ((0, 16),)),
        "expert_up": gaussian(keys[13], (D, EXPERTS * FF), D ** -0.5, 0.125, ((1, 16),)),
        "expert_down": gaussian(keys[14], (EXPERTS * FF, D), FF ** -0.5, 0.09375, ((0, 16),)),
    }


def attend_one(packed):
    query_row, key_rows, value_rows, key_self, value_self, valid = packed
    scale_factor = 1.0 / math.sqrt(HEAD_DIM)
    head_query = query_row.astype(jnp.float32).reshape(HEADS, HEAD_DIM)
    head_keys = key_rows.astype(jnp.float32).reshape(CACHE, HEADS, HEAD_DIM)
    head_values = value_rows.astype(jnp.float32).reshape(CACHE, HEADS, HEAD_DIM)
    scores = jnp.einsum('hd,chd->hc', head_query, head_keys) * scale_factor
    own_score = lax.optimization_barrier(jnp.sum(head_query * key_self.astype(jnp.float32).reshape(HEADS, HEAD_DIM), axis=1)) * scale_factor
    positions = jnp.arange(CACHE, dtype=jnp.int32)
    scores = jnp.where(positions[None, :] < valid, scores, -1e+30)
    top_score = jnp.maximum(lax.optimization_barrier(jnp.max(scores, axis=1)), own_score)
    weights = jnp.exp(scores - top_score[:, None])
    own_weight = jnp.exp(own_score - top_score)
    normalizer = lax.optimization_barrier(jnp.sum(weights, axis=1)) + own_weight
    weights = lax.optimization_barrier((weights / normalizer[:, None]).astype(jnp.bfloat16)).astype(jnp.float32)
    own_weight = lax.optimization_barrier((own_weight / normalizer).astype(jnp.bfloat16)).astype(jnp.float32)
    mixed_values = jnp.einsum('hc,chd->hd', weights, head_values)
    mixed_values = mixed_values + own_weight[:, None] * value_self.astype(jnp.float32).reshape(HEADS, HEAD_DIM)
    return mixed_values.reshape(D).astype(jnp.bfloat16)

def reference(query, key_new, value_new, key_cache, value_cache, lengths, hidden, routes, w_out, ln_gain, router, shared_up, shared_down, expert_up, expert_down):
    attended = lax.map(attend_one, (query, key_cache, value_cache, key_new, value_new, lengths))
    projected = jnp.dot(attended, w_out, preferred_element_type=jnp.float32).astype(jnp.bfloat16)
    projected = lax.optimization_barrier(projected).astype(jnp.float32)
    residual = hidden.astype(jnp.float32) + projected
    centered = residual - lax.optimization_barrier(jnp.mean(residual, axis=1, keepdims=True))
    variance = lax.optimization_barrier(jnp.mean(centered * centered, axis=1, keepdims=True))
    normed = (centered / jnp.sqrt(jnp.maximum(variance, 0.25)) * ln_gain.astype(jnp.float32)).astype(jnp.bfloat16)
    logits = jnp.dot(normed, router, preferred_element_type=jnp.float32)
    expert_ids = jnp.arange(EXPERTS, dtype=jnp.int32)
    chosen = lax.optimization_barrier(jnp.sum(jnp.where(routes[:, None] == expert_ids[None, :], logits, 0.0), axis=1))
    gate_value = jax.nn.sigmoid(chosen)
    shared_hidden = jax.nn.gelu(jnp.dot(normed, shared_up, preferred_element_type=jnp.float32), approximate=True).astype(jnp.bfloat16)
    shared_out = jnp.dot(shared_hidden, shared_down, preferred_element_type=jnp.float32)
    slot_ids = jnp.arange(CAP, dtype=jnp.int32)

    def one_expert(running, expert_id):
        member = routes == expert_id
        slot_rank = jnp.cumsum(member.astype(jnp.int32)) - 1
        placed = member[:, None] & (slot_rank[:, None] == slot_ids[None, :])
        picked = jnp.dot(placed.astype(jnp.bfloat16).T, normed, preferred_element_type=jnp.float32).astype(jnp.bfloat16)
        up_cols = lax.dynamic_slice_in_dim(expert_up, (expert_id * FF).astype(jnp.int32), FF, 1)
        down_rows = lax.dynamic_slice_in_dim(expert_down, (expert_id * FF).astype(jnp.int32), FF, 0)
        inner_act = jax.nn.gelu(jnp.dot(picked, up_cols, preferred_element_type=jnp.float32), approximate=True).astype(jnp.bfloat16)
        result = jnp.dot(inner_act, down_rows, preferred_element_type=jnp.float32)
        spread = placed.astype(jnp.float32) * gate_value[:, None]
        return (running + jnp.dot(spread, result, precision=lax.Precision.HIGHEST), None)
    expert_out, ignored = lax.scan(one_expert, jnp.zeros((S, D), jnp.float32), expert_ids)
    return (residual + shared_out + expert_out).astype(jnp.bfloat16)
```

```python
import functools
import math

import jax
import jax.numpy as jnp
from jax import lax
from jax.experimental import pallas as pl
from jax.experimental.pallas import tpu as pltpu
from jax.sharding import PartitionSpec as P

HEADS = 16
HEAD_DIM = 128
FF = 4096
EXPERTS = 32
CHUNK = 512
BLOCK = 256
MAX_SLOTS = 26
EARLY = 4
GROUP_COLS = 1024
MESH = pl.DeviceIdType.MESH
F32 = jnp.float32
BF16 = jnp.bfloat16


def gelu(v):
    return 0.5 * v * (1.0 + jnp.tanh(math.sqrt(2.0 / math.pi) * (v + 0.044715 * (v * v * v))))


def kernel(
    n,
    slots,
    lengths_ref,
    routes_ref,
    query_hbm,
    key_new_hbm,
    value_new_hbm,
    hidden_hbm,
    gain_hbm,
    keys_hbm,
    values_hbm,
    w_out_hbm,
    router_hbm,
    shared_up_hbm,
    shared_down_hbm,
    up_hbm,
    down_hbm,
    out_ref,
    query,
    key_new,
    value_new,
    hidden,
    gain,
    keys,
    values,
    w_out,
    router,
    shared_up,
    shared_down,
    ring,
    attended_all,
    hidden_all,
    unfold,
    projected_all,
    inner,
    normed_ref,
    gate_ref,
    shared_ref,
    own_ref,
    send_buf,
    recv_buf,
    local_sem,
    ring_sem,
    send_sem,
    recv_sem,
):
    me = lax.axis_index("expert")
    width = query.shape[1]
    units = up_hbm.shape[1]
    up_chunks = units // CHUNK
    piece = min(units, width)
    pieces = units // piece
    per = min(CHUNK // BLOCK, pieces)
    chunks_per_block = pieces // per
    blocks = width // BLOCK
    total = up_chunks + blocks * chunks_per_block

    barrier = pltpu.get_barrier_semaphore()

    def greet(off, carry):
        pl.semaphore_signal(
            barrier, inc=1, device_id={"expert": lax.rem(me + off, n)}, device_id_type=MESH
        )
        return carry

    lax.fori_loop(1, n, greet, 0)

    local = [
        pltpu.make_async_copy(src, dst, local_sem.at[i])
        for i, (src, dst) in enumerate(
            [
                (query_hbm, query),
                (key_new_hbm, key_new),
                (keys_hbm, keys),
                (values_hbm, values),
                (value_new_hbm, value_new),
                (hidden_hbm, hidden),
                (w_out_hbm, w_out),
                (gain_hbm, gain),
                (router_hbm, router),
                (shared_up_hbm, shared_up),
                (shared_down_hbm, shared_down),
            ]
        )
    ]
    (
        query_copy,
        key_new_copy,
        keys_copy,
        values_copy,
        value_new_copy,
        hidden_copy,
        w_out_copy,
        gain_copy,
        router_copy,
        shared_up_copy,
        shared_down_copy,
    ) = local

    def up_copy(chunk, slot):
        return pltpu.make_async_copy(
            up_hbm.at[:, pl.ds(pl.multiple_of(chunk * CHUNK, CHUNK), CHUNK)],
            ring.at[slot],
            ring_sem.at[slot],
        )

    def start_down(chunk, slot):
        block = chunk // chunks_per_block
        part = chunk - block * chunks_per_block
        for p in range(per):
            pltpu.make_async_copy(
                down_hbm.at[
                    pl.ds(pl.multiple_of((part * per + p) * piece, piece), piece),
                    pl.ds(pl.multiple_of(block * BLOCK, BLOCK), BLOCK),
                ],
                ring.at[slot, pl.ds(0, piece), pl.ds(p * BLOCK, BLOCK)],
                ring_sem.at[slot],
            ).start()

    def wait_down(slot):
        landed = ring.at[slot, pl.ds(0, piece), pl.ds(0, per * BLOCK)]
        pltpu.make_async_copy(landed, landed, ring_sem.at[slot]).wait()

    for copy in local[:7]:
        copy.start()
    for chunk in range(min(EARLY, up_chunks)):
        up_copy(chunk, chunk).start()

    rows = lax.broadcasted_iota(jnp.int32, (HEADS, width), 0)
    lanes = lax.broadcasted_iota(jnp.int32, (HEADS, width), 1)
    own_lane = lanes // HEAD_DIM == rows

    def fold(x):
        row = lax.broadcasted_iota(jnp.int32, (HEADS, HEAD_DIM), 0)
        taken = jnp.zeros((HEADS, HEAD_DIM), F32)
        for h in range(HEADS):
            taken = taken + jnp.where(row == h, x[:, h * HEAD_DIM : (h + 1) * HEAD_DIM], 0.0)
        return taken

    scale = 1.0 / math.sqrt(HEAD_DIM)
    query_copy.wait()
    key_new_copy.wait()
    spread_query = jnp.where(
        own_lane, jnp.broadcast_to(query[...].astype(F32), (HEADS, width)), 0.0
    )
    own_score = (
        jnp.sum(spread_query * key_new[...].astype(F32), axis=1, keepdims=True) * scale
    )
    spread_query = spread_query.astype(BF16)
    keys_copy.wait()
    scores = (
        lax.dot_general(
            spread_query, keys[...], (((1,), (1,)), ((), ())), preferred_element_type=F32
        )
        * scale
    )
    values_copy.wait()
    value_new_copy.wait()
    hidden_copy.wait()
    w_out_copy.wait()
    for copy in local[7:]:
        copy.start()
    for chunk in range(EARLY, min(slots, up_chunks)):
        up_copy(chunk, chunk).start()
    for chunk in range(up_chunks, slots):
        start_down(chunk - up_chunks, chunk)

    position = lax.broadcasted_iota(jnp.int32, scores.shape, 1)
    scores = jnp.where(position < lengths_ref[0], scores, -1e30)
    top = jnp.maximum(jnp.max(scores, axis=1, keepdims=True), own_score)
    weights = jnp.exp(scores - top)
    own_weight = jnp.exp(own_score - top)
    normalizer = jnp.sum(weights, axis=1, keepdims=True) + own_weight
    weights = (weights / normalizer).astype(BF16)
    own_weight = (own_weight / normalizer).astype(BF16).astype(F32)
    mixed = jnp.dot(weights, values[...], preferred_element_type=F32)
    mixed = mixed + own_weight * value_new[...].astype(F32)
    mine = pl.ds(pl.multiple_of(me * HEADS, HEADS), HEADS)
    attended_all[mine, :] = fold(mixed).astype(BF16)
    hidden_all[mine, :] = fold(
        jnp.broadcast_to(hidden[...].astype(F32), (HEADS, width))
    ).astype(BF16)

    pl.semaphore_wait(barrier, n - 1)

    def send_all(src, dst, sem):
        def send(off, carry):
            pltpu.make_async_remote_copy(
                src_ref=src,
                dst_ref=dst,
                send_sem=send_sem.at[sem],
                recv_sem=recv_sem.at[sem],
                device_id={"expert": lax.rem(me + off, n)},
                device_id_type=MESH,
            ).start()
            return carry

        lax.fori_loop(1, n, send, 0)

    def await_bytes(ref, sem):
        pltpu.make_async_copy(ref, ref, sem).wait()

    send_all(attended_all.at[mine, :], attended_all.at[mine, :], 0)
    send_all(hidden_all.at[mine, :], hidden_all.at[mine, :], 1)

    others = pl.ds(0, (n - 1) * HEADS)
    await_bytes(attended_all.at[others, :], recv_sem.at[0])
    unfold[...] = attended_all[...].astype(F32)
    attended = jnp.concatenate(
        [unfold[pl.ds(h, n, stride=HEADS), :].astype(BF16) for h in range(HEADS)], axis=1
    )
    projected = jnp.dot(attended, w_out[...], preferred_element_type=F32).astype(BF16)
    cols = projected.shape[1]
    my_cols = pl.ds(pl.multiple_of(me * cols, cols), cols)
    if cols % 128 == 0:
        projected_all[:, my_cols] = projected
        piece_ref = projected_all.at[:, my_cols]
        arrived = projected_all.at[:, pl.ds(0, (n - 1) * cols)]
    else:
        projected_all[me] = projected
        piece_ref = projected_all.at[me]
        arrived = projected_all.at[pl.ds(0, n - 1)]
    send_all(piece_ref, piece_ref, 2)
    await_bytes(hidden_all.at[others, :], recv_sem.at[1])
    unfold[...] = hidden_all[...].astype(F32)
    every_hidden = jnp.concatenate(
        [unfold[pl.ds(h, n, stride=HEADS), :] for h in range(HEADS)], axis=1
    )
    token = lax.broadcasted_iota(jnp.int32, (n, 1), 0)
    chosen_expert = jnp.zeros((n, 1), jnp.int32)
    for t in range(n):
        chosen_expert = jnp.where(token == t, routes_ref[t], chosen_expert)
    gain_copy.wait()
    router_copy.wait()
    await_bytes(arrived, recv_sem.at[2])
    if cols % 128 == 0:
        every_projected = projected_all[...].astype(F32)
    else:
        every_projected = jnp.concatenate(
            [projected_all[d].astype(F32) for d in range(n)], axis=1
        )
    residual = every_hidden + every_projected
    centered = residual - jnp.mean(residual, axis=1, keepdims=True)
    variance = jnp.mean(centered * centered, axis=1, keepdims=True)
    normed = (
        centered / jnp.sqrt(jnp.maximum(variance, 0.25)) * gain[...].astype(F32).reshape(1, width)
    ).astype(BF16)
    normed_ref[...] = normed
    own_ref[...] = jnp.sum(jnp.where(token == me, residual, 0.0), axis=0, keepdims=True)

    shared_up_copy.wait()
    shared_ref[...] = gelu(
        jnp.dot(normed_ref[...], shared_up[...], preferred_element_type=F32)
    ).astype(BF16)
    logits = lax.dot_general(
        normed_ref[...], router[...], (((1,), (1,)), ((), ())), preferred_element_type=F32
    )
    expert_ids = lax.broadcasted_iota(jnp.int32, logits.shape, 1)
    chosen = jnp.sum(jnp.where(chosen_expert == expert_ids, logits, 0.0), axis=1, keepdims=True)
    gate_ref[...] = 1.0 / (1.0 + jnp.exp(-chosen))

    def up_step(chunk, carry):
        up_copy(chunk, chunk).wait()
        act = gelu(jnp.dot(normed_ref[...], ring[chunk], preferred_element_type=F32))
        expert = (me * units + chunk * CHUNK) // FF
        inner[:, pl.ds(pl.multiple_of(chunk * CHUNK, CHUNK), CHUNK)] = jnp.where(
            chosen_expert == expert, act, 0.0
        ).astype(BF16)

        @pl.when(chunk + slots < total)
        def _():
            start_down(chunk + slots - up_chunks, chunk)

        return carry

    lax.fori_loop(0, up_chunks, up_step, 0)
    shared_down_copy.wait()

    group_rows = GROUP_COLS // 128
    groups = width // GROUP_COLS
    blocks_per_group = blocks // groups
    slab = n * group_rows

    for group in range(groups):

        def down_step(index, carry, group=group):
            block = group * blocks_per_group + index
            acc = jnp.zeros((n, BLOCK), F32)
            for part in range(chunks_per_block):
                chunk = up_chunks + block * chunks_per_block + part
                slot = lax.rem(chunk, slots)
                wait_down(slot)
                for p in range(per):
                    acc = acc + jnp.dot(
                        inner[:, pl.ds((part * per + p) * piece, piece)],
                        ring[slot, pl.ds(0, piece), pl.ds(p * BLOCK, BLOCK)],
                        preferred_element_type=F32,
                    )
            shared = jnp.dot(
                shared_ref[...],
                shared_down[:, pl.ds(pl.multiple_of(block * BLOCK, BLOCK), BLOCK)],
                preferred_element_type=F32,
            )
            terms = shared + gate_ref[...] * acc
            for k in range(BLOCK // 128):
                row = group * slab + index * (BLOCK // 128) + k
                send_buf[pl.ds(row, n, stride=group_rows), :] = terms[:, k * 128 : (k + 1) * 128]
            return carry

        lax.fori_loop(0, blocks_per_group, down_step, 0)
        mine_slab = pl.ds(
            pl.multiple_of(group * slab + me * group_rows, group_rows), group_rows
        )

        def send_terms(off, carry, group=group, mine_slab=mine_slab):
            peer = lax.rem(me + off, n)
            pltpu.make_async_remote_copy(
                src_ref=send_buf.at[
                    pl.ds(pl.multiple_of(group * slab + peer * group_rows, group_rows), group_rows), :
                ],
                dst_ref=recv_buf.at[mine_slab, :],
                send_sem=send_sem.at[3 + group],
                recv_sem=recv_sem.at[3 + group],
                device_id={"expert": peer},
                device_id_type=MESH,
            ).start()
            return carry

        lax.fori_loop(1, n, send_terms, 0)
        recv_buf[mine_slab, :] = send_buf[mine_slab, :]

    for group in range(groups):
        landed = recv_buf.at[pl.ds(group * slab, (n - 1) * group_rows), :]
        await_bytes(landed, recv_sem.at[3 + group])
        summed = jnp.zeros((group_rows, 128), F32)
        for d in range(n):
            summed = summed + recv_buf[pl.ds(group * slab + d * group_rows, group_rows), :]
        for j in range(group_rows):
            where = pl.ds(group * GROUP_COLS + j * 128, 128)
            out_ref[:, where] = (own_ref[:, where] + summed[j : j + 1, :]).astype(out_ref.dtype)

    await_bytes(attended_all.at[others, :], send_sem.at[0])
    await_bytes(hidden_all.at[others, :], send_sem.at[1])
    await_bytes(arrived, send_sem.at[2])
    for group in range(groups):
        sent = send_buf.at[pl.ds(group * slab, (n - 1) * group_rows), :]
        await_bytes(sent, send_sem.at[3 + group])


def solution(mesh):
    n = mesh.shape["expert"]

    def body(
        query,
        key_new,
        value_new,
        key_cache,
        value_cache,
        lengths,
        hidden,
        routes,
        w_out,
        ln_gain,
        router,
        shared_up,
        shared_down,
        expert_up,
        expert_down,
    ):
        assert query.shape[0] == 1
        width = query.shape[1]
        units = expert_up.shape[1]
        cache = key_cache.shape[1]
        shared_units = shared_up.shape[1]
        cols = w_out.shape[1]
        piece = min(units, width)
        per = min(CHUNK // BLOCK, units // piece)
        total = units // CHUNK + (width // BLOCK) * (units // piece // per)
        slots = min(MAX_SLOTS, total)
        groups = width // GROUP_COLS
        flat = (width // GROUP_COLS) * n * (GROUP_COLS // 128)
        gathered = (n, width) if cols % 128 == 0 else (n, n, cols)
        vmem = pltpu.VMEM
        smem = pl.BlockSpec(memory_space=pltpu.SMEM)
        hbm = pl.BlockSpec(memory_space=pl.ANY)
        return pl.pallas_call(
            functools.partial(kernel, n, slots),
            out_shape=jax.ShapeDtypeStruct((1, width), BF16),
            in_specs=[smem] * 2 + [hbm] * 13,
            out_specs=pl.BlockSpec(memory_space=pltpu.VMEM),
            scratch_shapes=[
                vmem((1, width), BF16),
                vmem((1, width), BF16),
                vmem((1, width), BF16),
                vmem((1, width), BF16),
                vmem((width,), BF16),
                vmem((cache, width), BF16),
                vmem((cache, width), BF16),
                vmem((width, cols), BF16),
                vmem((EXPERTS, width), BF16),
                vmem((width, shared_units), BF16),
                vmem((shared_units, width), BF16),
                vmem((slots, width, CHUNK), BF16),
                vmem((n * HEADS, HEAD_DIM), BF16),
                vmem((n * HEADS, HEAD_DIM), BF16),
                vmem((n * HEADS, HEAD_DIM), F32),
                vmem(gathered, BF16),
                vmem((n, units), BF16),
                vmem((n, width), BF16),
                vmem((n, 1), F32),
                vmem((n, shared_units), BF16),
                vmem((1, width), F32),
                vmem((flat, 128), F32),
                vmem((flat, 128), F32),
                pltpu.SemaphoreType.DMA((11,)),
                pltpu.SemaphoreType.DMA((slots,)),
                pltpu.SemaphoreType.DMA((3 + groups,)),
                pltpu.SemaphoreType.DMA((3 + groups,)),
            ],
            compiler_params=pltpu.CompilerParams(
                collective_id=0, has_side_effects=True, vmem_limit_bytes=66_900_000
            ),
        )(
            lengths,
            routes,
            query,
            key_new,
            value_new,
            hidden,
            ln_gain,
            key_cache.reshape(cache, width),
            value_cache.reshape(cache, width),
            w_out,
            router.T,
            shared_up,
            shared_down,
            expert_up,
            expert_down,
        )

    rows = P(("group", "expert"), None)
    placed = (
        rows,
        rows,
        rows,
        P(("group", "expert"), None, None),
        P(("group", "expert"), None, None),
        P(("group", "expert")),
        rows,
        P("group"),
        P(None, "expert"),
        P(),
        P(),
        P(None, "expert"),
        P("expert", None),
        P(None, "expert"),
        P("expert", None),
    )
    return jax.shard_map(body, mesh=mesh, in_specs=placed, out_specs=rows, check_vma=False)
```

```python
import functools
import math

import jax
import jax.numpy as jnp
from jax import lax
from jax.experimental import pallas as pl
from jax.experimental.pallas import tpu as pltpu
from jax.sharding import PartitionSpec as P

HEADS = 16
HEAD_DIM = 128
FF = 4096
EXPERTS = 32
CHUNK = 512
BLOCK = 512
MAX_SLOTS = 26
EARLY = 3
PRIORITY = 1
TOGETHER = 4
JOINT = 1
GROUP_COLS = 1024
MESH = pl.DeviceIdType.MESH
F32 = jnp.float32
BF16 = jnp.bfloat16


def gelu(v):
    return 0.5 * v * (1.0 + jnp.tanh(math.sqrt(2.0 / math.pi) * (v + 0.044715 * (v * v * v))))


def kernel(
    n,
    slots,
    lengths_ref,
    routes_ref,
    query_hbm,
    key_new_hbm,
    value_new_hbm,
    hidden_hbm,
    gain_hbm,
    keys_hbm,
    values_hbm,
    w_out_hbm,
    router_hbm,
    shared_up_hbm,
    shared_down_hbm,
    up_hbm,
    down_hbm,
    out_ref,
    query,
    key_new,
    value_new,
    hidden,
    gain,
    keys,
    values,
    w_out,
    router,
    shared_up,
    shared_down,
    ring,
    attended_all,
    hidden_all,
    unfold,
    projected_all,
    inner,
    normed_ref,
    gate_ref,
    shared_ref,
    own_ref,
    send_buf,
    recv_buf,
    local_sem,
    ring_sem,
    send_sem,
    recv_sem,
):
    me = lax.axis_index("expert")
    width = query.shape[1]
    units = up_hbm.shape[1]
    up_chunks = units // CHUNK
    piece = min(units, width)
    pieces = units // piece
    blocks = width // BLOCK
    total = up_chunks + blocks * pieces

    barrier = pltpu.get_barrier_semaphore()

    local = [
        pltpu.make_async_copy(src, dst, local_sem.at[i])
        for i, (src, dst) in enumerate(
            [
                (query_hbm, query),
                (key_new_hbm, key_new),
                (keys_hbm, keys),
                (values_hbm, values),
                (value_new_hbm, value_new),
                (hidden_hbm, hidden),
                (w_out_hbm, w_out),
                (gain_hbm, gain),
                (router_hbm, router),
                (shared_up_hbm, shared_up),
                (shared_down_hbm, shared_down),
            ]
        )
    ]
    (
        query_copy,
        key_new_copy,
        keys_copy,
        values_copy,
        value_new_copy,
        hidden_copy,
        w_out_copy,
        gain_copy,
        router_copy,
        shared_up_copy,
        shared_down_copy,
    ) = local

    def up_copy(chunk, slot):
        return pltpu.make_async_copy(
            up_hbm.at[:, pl.ds(pl.multiple_of(chunk * CHUNK, CHUNK), CHUNK)],
            ring.at[slot],
            ring_sem.at[slot],
        )

    def down_copy(chunk, slot):
        block = chunk // pieces
        part = chunk - block * pieces
        return pltpu.make_async_copy(
            down_hbm.at[
                pl.ds(pl.multiple_of(part * piece, piece), piece),
                pl.ds(pl.multiple_of(block * BLOCK, BLOCK), BLOCK),
            ],
            ring.at[slot, pl.ds(0, piece), :],
            ring_sem.at[slot],
        )

    def chunk_copy(chunk):
        if chunk < up_chunks:
            return up_copy(chunk, chunk)
        return down_copy(chunk - up_chunks, chunk)

    issued = 0

    def start_chunks(last):
        nonlocal issued
        while issued < min(last, slots):
            chunk_copy(issued).start(priority=PRIORITY)
            issued += 1

    for copy in (query_copy, key_new_copy, keys_copy, values_copy, value_new_copy, hidden_copy, w_out_copy):
        copy.start()
    start_chunks(EARLY)

    def greet(off, carry):
        pl.semaphore_signal(
            barrier, inc=1, device_id={"expert": lax.rem(me + off, n)}, device_id_type=MESH
        )
        return carry

    lax.fori_loop(1, n, greet, 0)

    rows = lax.broadcasted_iota(jnp.int32, (HEADS, width), 0)
    lanes = lax.broadcasted_iota(jnp.int32, (HEADS, width), 1)
    own_lane = lanes // HEAD_DIM == rows

    def fold(x):
        row = lax.broadcasted_iota(jnp.int32, (HEADS, HEAD_DIM), 0)
        taken = jnp.zeros((HEADS, HEAD_DIM), F32)
        for h in range(HEADS):
            taken = taken + jnp.where(row == h, x[:, h * HEAD_DIM : (h + 1) * HEAD_DIM], 0.0)
        return taken

    scale = 1.0 / math.sqrt(HEAD_DIM)
    query_copy.wait()
    key_new_copy.wait()
    spread_query = jnp.where(
        own_lane, jnp.broadcast_to(query[...].astype(F32), (HEADS, width)), 0.0
    )
    own_score = (
        jnp.sum(spread_query * key_new[...].astype(F32), axis=1, keepdims=True) * scale
    )
    spread_query = spread_query.astype(BF16)
    keys_copy.wait()
    scores = (
        lax.dot_general(
            spread_query, keys[...], (((1,), (1,)), ((), ())), preferred_element_type=F32
        )
        * scale
    )
    values_copy.wait()
    value_new_copy.wait()
    hidden_copy.wait()
    for copy in local[7:]:
        copy.start()
    start_chunks(slots)

    position = lax.broadcasted_iota(jnp.int32, scores.shape, 1)
    scores = jnp.where(position < lengths_ref[0], scores, -1e30)
    top = jnp.maximum(jnp.max(scores, axis=1, keepdims=True), own_score)
    weights = jnp.exp(scores - top)
    own_weight = jnp.exp(own_score - top)
    normalizer = jnp.sum(weights, axis=1, keepdims=True) + own_weight
    weights = (weights / normalizer).astype(BF16)
    own_weight = (own_weight / normalizer).astype(BF16).astype(F32)
    mixed = jnp.dot(weights, values[...], preferred_element_type=F32)
    mixed = mixed + own_weight * value_new[...].astype(F32)
    mine = pl.ds(pl.multiple_of(me * HEADS, HEADS), HEADS)
    attended_all[mine, :] = fold(mixed).astype(BF16)
    hidden_all[mine, :] = fold(
        jnp.broadcast_to(hidden[...].astype(F32), (HEADS, width))
    ).astype(BF16)

    pl.semaphore_wait(barrier, n - 1)

    def send_all(src, dst, sem):
        def send(off, carry):
            pltpu.make_async_remote_copy(
                src_ref=src,
                dst_ref=dst,
                send_sem=send_sem.at[sem],
                recv_sem=recv_sem.at[sem],
                device_id={"expert": lax.rem(me + off, n)},
                device_id_type=MESH,
            ).start()
            return carry

        lax.fori_loop(1, n, send, 0)

    def await_bytes(ref, sem):
        pltpu.make_async_copy(ref, ref, sem).wait()

    send_all(attended_all.at[mine, :], attended_all.at[mine, :], 0)
    send_all(hidden_all.at[mine, :], hidden_all.at[mine, :], 1)

    others = pl.ds(0, (n - 1) * HEADS)
    await_bytes(attended_all.at[others, :], recv_sem.at[0])
    unfold[...] = attended_all[...].astype(F32)
    attended = jnp.concatenate(
        [unfold[pl.ds(h, n, stride=HEADS), :].astype(BF16) for h in range(HEADS)], axis=1
    )
    w_out_copy.wait()
    projected = jnp.dot(attended, w_out[...], preferred_element_type=F32).astype(BF16)
    cols = projected.shape[1]
    my_cols = pl.ds(pl.multiple_of(me * cols, cols), cols)
    if cols % 128 == 0:
        projected_all[:, my_cols] = projected
        piece_ref = projected_all.at[:, my_cols]
        arrived = projected_all.at[:, pl.ds(0, (n - 1) * cols)]
    else:
        projected_all[me] = projected
        piece_ref = projected_all.at[me]
        arrived = projected_all.at[pl.ds(0, n - 1)]
    send_all(piece_ref, piece_ref, 2)
    await_bytes(hidden_all.at[others, :], recv_sem.at[1])
    unfold[...] = hidden_all[...].astype(F32)
    every_hidden = jnp.concatenate(
        [unfold[pl.ds(h, n, stride=HEADS), :] for h in range(HEADS)], axis=1
    )
    token = lax.broadcasted_iota(jnp.int32, (n, 1), 0)
    chosen_expert = jnp.zeros((n, 1), jnp.int32)
    for t in range(n):
        chosen_expert = jnp.where(token == t, routes_ref[t], chosen_expert)
    gain_copy.wait()
    router_copy.wait()
    await_bytes(arrived, recv_sem.at[2])
    if cols % 128 == 0:
        every_projected = projected_all[...].astype(F32)
    else:
        every_projected = jnp.concatenate(
            [projected_all[d].astype(F32) for d in range(n)], axis=1
        )
    residual = every_hidden + every_projected
    centered = residual - jnp.mean(residual, axis=1, keepdims=True)
    variance = jnp.mean(centered * centered, axis=1, keepdims=True)
    normed = (
        centered / jnp.sqrt(jnp.maximum(variance, 0.25)) * gain[...].astype(F32).reshape(1, width)
    ).astype(BF16)
    normed_ref[...] = normed
    own_ref[...] = jnp.sum(jnp.where(token == me, residual, 0.0), axis=0, keepdims=True)

    shared_up_copy.wait()
    shared_ref[...] = gelu(
        jnp.dot(normed_ref[...], shared_up[...], preferred_element_type=F32)
    ).astype(BF16)
    logits = lax.dot_general(
        normed_ref[...], router[...], (((1,), (1,)), ((), ())), preferred_element_type=F32
    )
    expert_ids = lax.broadcasted_iota(jnp.int32, logits.shape, 1)
    chosen = jnp.sum(jnp.where(chosen_expert == expert_ids, logits, 0.0), axis=1, keepdims=True)
    gate_ref[...] = 1.0 / (1.0 + jnp.exp(-chosen))

    together = math.gcd(TOGETHER, up_chunks)

    def up_step(step, carry):
        chunks = [step * together + i for i in range(together)]
        for chunk in chunks:
            up_copy(chunk, chunk).wait()
        for chunk in chunks:
            act = gelu(jnp.dot(normed_ref[...], ring[chunk], preferred_element_type=F32))
            expert = (me * units + chunk * CHUNK) // FF
            inner[:, pl.ds(pl.multiple_of(chunk * CHUNK, CHUNK), CHUNK)] = jnp.where(
                chosen_expert == expert, act, 0.0
            ).astype(BF16)
        for chunk in chunks:

            @pl.when(chunk + slots < total)
            def _(chunk=chunk):
                down_copy(chunk + slots - up_chunks, chunk).start(priority=PRIORITY)

        return carry

    lax.fori_loop(0, up_chunks // together, up_step, 0)
    shared_down_copy.wait()

    group_rows = GROUP_COLS // 128
    groups = width // GROUP_COLS
    blocks_per_group = blocks // groups
    slab = n * group_rows

    for group in range(groups):

        def down_step(index, carry, group=group):
            block = group * blocks_per_group + index
            acc = jnp.zeros((n, BLOCK), F32)
            first = up_chunks + block * pieces
            held = [lax.rem(first + part, slots) for part in range(pieces)]
            for part in range(pieces):
                if part % JOINT == 0:
                    for later in range(part, min(part + JOINT, pieces)):
                        down_copy(first + later - up_chunks, held[later]).wait()
                acc = acc + jnp.dot(
                    inner[:, pl.ds(part * piece, piece)],
                    ring[held[part], pl.ds(0, piece), :],
                    preferred_element_type=F32,
                )
            shared = jnp.dot(
                shared_ref[...],
                shared_down[:, pl.ds(pl.multiple_of(block * BLOCK, BLOCK), BLOCK)],
                preferred_element_type=F32,
            )
            terms = shared + gate_ref[...] * acc
            for k in range(BLOCK // 128):
                row = group * slab + index * (BLOCK // 128) + k
                send_buf[pl.ds(row, n, stride=group_rows), :] = terms[:, k * 128 : (k + 1) * 128]
            return carry

        lax.fori_loop(0, blocks_per_group, down_step, 0)
        mine_slab = pl.ds(
            pl.multiple_of(group * slab + me * group_rows, group_rows), group_rows
        )

        def send_terms(off, carry, group=group, mine_slab=mine_slab):
            peer = lax.rem(me + off, n)
            pltpu.make_async_remote_copy(
                src_ref=send_buf.at[
                    pl.ds(pl.multiple_of(group * slab + peer * group_rows, group_rows), group_rows), :
                ],
                dst_ref=recv_buf.at[mine_slab, :],
                send_sem=send_sem.at[3 + group],
                recv_sem=recv_sem.at[3 + group],
                device_id={"expert": peer},
                device_id_type=MESH,
            ).start()
            return carry

        lax.fori_loop(1, n, send_terms, 0)
        recv_buf[mine_slab, :] = send_buf[mine_slab, :]

    for group in range(groups):
        landed = recv_buf.at[pl.ds(group * slab, (n - 1) * group_rows), :]
        await_bytes(landed, recv_sem.at[3 + group])
        summed = jnp.zeros((group_rows, 128), F32)
        for d in range(n):
            summed = summed + recv_buf[pl.ds(group * slab + d * group_rows, group_rows), :]
        for j in range(group_rows):
            where = pl.ds(group * GROUP_COLS + j * 128, 128)
            out_ref[:, where] = (own_ref[:, where] + summed[j : j + 1, :]).astype(out_ref.dtype)

    await_bytes(attended_all.at[others, :], send_sem.at[0])
    await_bytes(hidden_all.at[others, :], send_sem.at[1])
    await_bytes(arrived, send_sem.at[2])
    for group in range(groups):
        sent = send_buf.at[pl.ds(group * slab, (n - 1) * group_rows), :]
        await_bytes(sent, send_sem.at[3 + group])


def solution(mesh):
    n = mesh.shape["expert"]

    def body(
        query,
        key_new,
        value_new,
        key_cache,
        value_cache,
        lengths,
        hidden,
        routes,
        w_out,
        ln_gain,
        router,
        shared_up,
        shared_down,
        expert_up,
        expert_down,
    ):
        assert query.shape[0] == 1
        width = query.shape[1]
        units = expert_up.shape[1]
        cache = key_cache.shape[1]
        shared_units = shared_up.shape[1]
        cols = w_out.shape[1]
        piece = min(units, width)
        total = units // CHUNK + (width // BLOCK) * (units // piece)
        slots = min(MAX_SLOTS, total)
        groups = width // GROUP_COLS
        flat = (width // GROUP_COLS) * n * (GROUP_COLS // 128)
        gathered = (n, width) if cols % 128 == 0 else (n, n, cols)
        vmem = pltpu.VMEM
        smem = pl.BlockSpec(memory_space=pltpu.SMEM)
        hbm = pl.BlockSpec(memory_space=pl.ANY)
        return pl.pallas_call(
            functools.partial(kernel, n, slots),
            out_shape=pltpu.VMEM((1, width), BF16),
            in_specs=[smem] * 2 + [hbm] * 13,
            out_specs=pl.BlockSpec(memory_space=pltpu.VMEM),
            scratch_shapes=[
                vmem((1, width), BF16),
                vmem((1, width), BF16),
                vmem((1, width), BF16),
                vmem((1, width), BF16),
                vmem((width,), BF16),
                vmem((cache, width), BF16),
                vmem((cache, width), BF16),
                vmem((width, cols), BF16),
                vmem((EXPERTS, width), BF16),
                vmem((width, shared_units), BF16),
                vmem((shared_units, width), BF16),
                vmem((slots, width, CHUNK), BF16),
                vmem((n * HEADS, HEAD_DIM), BF16),
                vmem((n * HEADS, HEAD_DIM), BF16),
                vmem((n * HEADS, HEAD_DIM), F32),
                vmem(gathered, BF16),
                vmem((n, units), BF16),
                vmem((n, width), BF16),
                vmem((n, 1), F32),
                vmem((n, shared_units), BF16),
                vmem((1, width), F32),
                vmem((flat, 128), F32),
                vmem((flat, 128), F32),
                pltpu.SemaphoreType.DMA((11,)),
                pltpu.SemaphoreType.DMA((slots,)),
                pltpu.SemaphoreType.DMA((3 + groups,)),
                pltpu.SemaphoreType.DMA((3 + groups,)),
            ],
            compiler_params=pltpu.CompilerParams(
                collective_id=0, has_side_effects=True, vmem_limit_bytes=66_900_000
            ),
        )(
            lengths,
            routes,
            query,
            key_new,
            value_new,
            hidden,
            ln_gain,
            key_cache.reshape(cache, width),
            value_cache.reshape(cache, width),
            w_out,
            router.T,
            shared_up,
            shared_down,
            expert_up,
            expert_down,
        )

    rows = P(("group", "expert"), None)
    placed = (
        rows,
        rows,
        rows,
        P(("group", "expert"), None, None),
        P(("group", "expert"), None, None),
        P(("group", "expert")),
        rows,
        P("group"),
        P(None, "expert"),
        P(),
        P(),
        P(None, "expert"),
        P("expert", None),
        P(None, "expert"),
        P("expert", None),
    )
    return jax.shard_map(body, mesh=mesh, in_specs=placed, out_specs=rows, check_vma=False)
```
